16 devices in a mesh: dp: 2 (over y, z), tp: 8 (over x, core).
Axes of the slice: x: 4, y: 2, z: 1, core: 2. Of those that a mesh axis runs over, the one named last changes fastest.
The devices are a block of a 4x4x8 slice.
Arguments:
- x: bfloat16 [8192, 2048], P(('dp', 'tp')), parts along dimension 0
- w_gate: bfloat16 [2048, 8192], P(None, 'tp')
- w_up: bfloat16 [2048, 8192], P(None, 'tp')
- w_down: bfloat16 [8192, 2048], P('tp')
Outputs:
- output: bfloat16 [8192, 2048], P(('dp', 'tp')), parts along dimension 0
There are 2 independent parts. The reference program is written for one: setup_inputs(seed, part) draws one part's arguments, and reference() takes and returns one part's arrays. A program takes and returns all parts, laid end to end along the dimension named above; an argument that names none is the same for every part.
All inputs are finite; a program needn't handle non-finite values.
Results may differ from the reference program's by a relative error of at most 0.016.
Values are sent between devices in bfloat16 or wider.
A program may use at most 768 MiB of HBM per device.

```python
import jax
import jax.numpy as jnp

ROWS = 4096
D = 2048
FF = 8192


def setup_inputs(seed: int = 0, part: int = 0) -> dict:
    kx, kg, ku, kd = jax.random.split(jax.random.key(seed), 4)
    drawn = {
        "x": jax.random.normal(jax.random.fold_in(kx, part), (ROWS, D), jnp.float32),
        "w_gate": jax.random.normal(kg, (D, FF), jnp.float32) * D**-0.5,
        "w_up": jax.random.normal(ku, (D, FF), jnp.float32) * D**-0.5,
        "w_down": jax.random.normal(kd, (FF, D), jnp.float32) * FF**-0.5,
    }
    return {k: v.astype(jnp.bfloat16) for k, v in drawn.items()}


def reference(x, w_gate, w_up, w_down):
    gate = jnp.dot(x, w_gate, preferred_element_type=jnp.float32)
    up = jnp.dot(x, w_up, preferred_element_type=jnp.float32)
    hidden = (jax.nn.silu(gate) * up).astype(jnp.bfloat16)
    return jnp.dot(hidden, w_down, preferred_element_type=jnp.float32).astype(jnp.bfloat16)
```

```python
import functools

import jax
import jax.numpy as jnp
from jax import lax
from jax.experimental import pallas as pl
from jax.experimental.pallas import tpu as pltpu
from jax.sharding import PartitionSpec as P

F32 = jnp.float32
CORES = 2
PIECES = 2
ACC_PIECES = 4
TILE = 256

SLOTS = 8
STEPS = 2 * SLOTS


def kernel(
    n, x_hbm, wg_hbm, wu_hbm, wd_hbm, y_hbm,
    x_all, wg, wu, wd, hidden, acc, terms, partner_terms, arrived, staged,
    load_sem, ag_send, ag_recv, relay_send, relay_recv, pt_send, pt_recv,
    far_send, far_recv, plain_send, plain_recv, sum_send, sum_recv, out_sem,
):
    half, depth = x_all.shape[1:]
    me = lax.axis_index("tp")
    right = {"tp": lax.rem(me + CORES, n)}
    left = {"tp": lax.rem(me + n - CORES, n)}
    partner = {"tp": me + 1 - 2 * lax.rem(me, CORES)}
    part = half // PIECES
    spart = half // ACC_PIECES

    def rows(p, size):
        return pl.ds(p * size, size)

    def remote(src, dst, send, recv, device):
        return pltpu.make_async_remote_copy(
            src_ref=src, dst_ref=dst, send_sem=send, recv_sem=recv,
            device_id=device, device_id_type=pl.DeviceIdType.MESH,
        )

    def mine(slot):
        return 2 * slot + 1

    moves = [(0, 2, right), (1, 3, left), (2, 4, right), (3, 5, left), (0, 6, left), (1, 7, right)]

    def gather(m, p):
        src, dst, device = moves[m]
        return remote(
            x_all.at[mine(src), rows(p, part)], x_all.at[mine(dst), rows(p, part)],
            ag_send.at[m, p], ag_recv.at[m, p], device,
        )

    def relay(slot, p):
        return remote(
            x_all.at[mine(slot), rows(p, part)], x_all.at[2 * slot, rows(p, part)],
            relay_send.at[slot, p], relay_recv.at[slot, p], partner,
        )

    def partner_term(slot):
        return remote(
            x_all.at[2 * slot], partner_terms.at[slot], pt_send.at[slot], pt_recv.at[slot], partner
        )

    def far_term(h, p):
        return remote(
            terms.at[2 + h, rows(p, part)], arrived.at[h, rows(p, part)],
            far_send.at[h, p], far_recv.at[h, p], (right, left)[h],
        )

    def plain_term(h, p):
        return remote(
            terms.at[h, rows(p, part)], arrived.at[2 + h, rows(p, part)],
            plain_send.at[h, p], plain_recv.at[h, p], (left, right)[h],
        )

    def sum_term(h, p):
        return remote(
            terms.at[4 + h, rows(p, spart)], arrived.at[4 + h, rows(p, spart)],
            sum_send.at[h, p], sum_recv.at[h, p], (right, left)[h],
        )

    def out(h, p):
        return pltpu.make_async_copy(
            staged.at[h, rows(p, spart)], y_hbm.at[rows(h * ACC_PIECES + p, spart)], out_sem.at[h, p]
        )

    own = [pltpu.make_async_copy(x_hbm.at[rows(h, half)], x_all.at[mine(h)], load_sem.at[h]) for h in range(2)]
    weights = [
        pltpu.make_async_copy(src, dst, load_sem.at[2 + i])
        for i, (src, dst) in enumerate(((wg_hbm, wg), (wu_hbm, wu), (wd_hbm, wd)))
    ]
    for c in own + weights:
        c.start()
    barrier = pltpu.get_barrier_semaphore()
    for device in (right, left, partner):
        pl.semaphore_signal(barrier, inc=1, device_id=device, device_id_type=pl.DeviceIdType.MESH)
    pl.semaphore_wait(barrier, 3)
    for h in range(2):
        own[h].wait()
        for p in range(PIECES):
            gather(h, p).start()
    for h in range(2):
        for p in range(PIECES):
            relay(h, p).start()
    for c in weights:
        c.wait()

    def arrive(slots, p):
        for slot in slots:
            gather(slot - 2, p).wait_recv()
            if slot in (2, 3):
                gather(slot, p).start()
            relay(slot, p).start()

    def relayed(slot):
        for p in range(PIECES):
            relay(slot, p).wait_recv()

    def start_near2():
        for m in (4, 5):
            for p in range(PIECES):
                gather(m, p).start()

    before = {
        0: [lambda: relayed(0)],
        2: [lambda: relayed(1)],
        4: [lambda: arrive((2, 3), 0), lambda: arrive((2, 3), 1), start_near2, lambda: relayed(2)],
        6: [lambda: relayed(3)],
        8: [lambda: arrive((4, 5), 0), lambda: arrive((4, 5), 1), lambda: relayed(4)],
        10: [lambda: relayed(5)],
        12: [lambda: arrive((6, 7), 0), lambda: arrive((6, 7), 1), lambda: relayed(6)],
        14: [lambda: relayed(7)],
    }

    def add_rows(start, size, srcs, dst):
        chunk = 32

        @pl.loop(0, size // chunk)
        def _(i):
            r = pl.ds(pl.multiple_of(start + i * chunk, chunk), chunk)
            total = srcs[0][r, :].astype(F32)
            for s in srcs[1:]:
                total += s[r, :].astype(F32)
            dst[r, :] = total.astype(dst.dtype)

    def finish_far(h):
        partner_term(4 + h).wait_recv()
        for p in range(PIECES):
            add_rows(p * part, part, [acc.at[0], partner_terms.at[4 + h]], terms.at[2 + h])
            far_term(h, p).start()

    def finish_plain(h):
        partner_term(2 + h).wait_recv()
        add_rows(0, half, [acc.at[0], partner_terms.at[2 + h]], terms.at[h])

    def start_plain():
        for h in range(2):
            for p in range(PIECES):
                plain_term(h, p).start()

    after = {
        5: [lambda: finish_plain(0)],
        7: [lambda: finish_plain(1)],
        9: [lambda: finish_far(0)],
        11: [lambda: finish_far(1), start_plain],
    }

    def step(t, carry):
        for at, actions in before.items():

            @pl.when(t == at)
            def _():
                for a in actions:
                    a()

        rows_in = x_all.at[t]
        for c in range(0, hidden.shape[1], TILE):
            cols = pl.ds(c, TILE)
            gate = jnp.dot(rows_in[...], wg[:, cols], preferred_element_type=F32)
            up = jnp.dot(rows_in[...], wu[:, cols], preferred_element_type=F32)
            hidden[:, cols] = (jax.nn.silu(gate) * up).astype(hidden.dtype)
        slot = t // 2
        to = (t % 2) * (jnp.where(slot < 2, slot + 1, 0) + jnp.where(slot > 5, slot - 3, 0))
        for c in range(0, depth, TILE):
            cols = pl.ds(c, TILE)
            acc[to, :, cols] = jnp.dot(hidden[...], wd[:, cols], preferred_element_type=F32)

        @pl.when(t % 2 == 0)
        def _():
            add_rows(0, half, [acc.at[0]], x_all.at[t])
            partner_term(slot).start()

        for at, actions in after.items():

            @pl.when(t == at)
            def _():
                for a in actions:
                    a()

        return carry

    lax.fori_loop(0, STEPS, step, 0)

    for h in range(2):
        partner_term(6 + h).wait_recv()
    for p in range(PIECES):
        for h in range(2):
            far_term(h, p).wait_recv()
            ratio = ACC_PIECES // PIECES
            for q in range(p * ratio, (p + 1) * ratio):
                add_rows(q * spart, spart, [acc.at[3 + h], partner_terms.at[6 + h], arrived.at[h]], terms.at[4 + h])
                sum_term(h, q).start()
    for h in range(2):
        partner_term(h).wait_recv()
        for p in range(PIECES):
            plain_term(h, p).wait_recv()
        add_rows(0, half, [acc.at[1 + h], partner_terms.at[h], arrived.at[2 + h]], acc.at[1 + h])
    for p in range(ACC_PIECES):
        for h in range(2):
            sum_term(h, p).wait_recv()
            add_rows(p * spart, spart, [acc.at[1 + h], arrived.at[4 + h]], staged.at[h])
            out(h, p).start()

    for p in range(ACC_PIECES):
        for h in range(2):
            out(h, p).wait()
            sum_term(h, p).wait_send()
    for p in range(PIECES):
        for m in range(6):
            gather(m, p).wait_send()
        for slot in range(SLOTS):
            relay(slot, p).wait_send()
        for h in range(2):
            far_term(h, p).wait_send()
            plain_term(h, p).wait_send()
    for slot in range(SLOTS):
        partner_term(slot).wait_send()


def solution(mesh):
    n = mesh.shape["tp"]

    def step(x, w_gate, w_up, w_down):
        rows, depth = x.shape
        width = w_gate.shape[1]
        half = rows // 2
        dma = pltpu.SemaphoreType.DMA
        bf16 = jnp.bfloat16
        return pl.pallas_call(
            functools.partial(kernel, n),
            out_shape=jax.ShapeDtypeStruct((rows, depth), bf16),
            in_specs=[pl.BlockSpec(memory_space=pl.ANY)] * 4,
            out_specs=pl.BlockSpec(memory_space=pl.ANY),
            scratch_shapes=[
                pltpu.VMEM((STEPS, half, depth), bf16),
                pltpu.VMEM((depth, width), bf16),
                pltpu.VMEM((depth, width), bf16),
                pltpu.VMEM((width, depth), bf16),
                pltpu.VMEM((half, width), bf16),
                pltpu.VMEM((5, half, depth), F32),
                pltpu.VMEM((6, half, depth), bf16),
                pltpu.VMEM((SLOTS, half, depth), bf16),
                pltpu.VMEM((6, half, depth), bf16),
                pltpu.VMEM((2, half, depth), bf16),
                dma((5,)),
                dma((6, PIECES)),
                dma((6, PIECES)),
                dma((SLOTS, PIECES)),
                dma((SLOTS, PIECES)),
                dma((SLOTS,)),
                dma((SLOTS,)),
                dma((2, PIECES)),
                dma((2, PIECES)),
                dma((2, PIECES)),
                dma((2, PIECES)),
                dma((2, ACC_PIECES)),
                dma((2, ACC_PIECES)),
                dma((2, ACC_PIECES)),
            ],
            compiler_params=pltpu.CompilerParams(
                collective_id=0, has_side_effects=True, vmem_limit_bytes=67_000_000
            ),
        )(x, w_gate, w_up, w_down)

    return jax.shard_map(
        step,
        mesh=mesh,
        in_specs=(P(("dp", "tp"), None), P(None, "tp"), P(None, "tp"), P("tp", None)),
        out_specs=P(("dp", "tp"), None),
        check_vma=False,
    )
```

```python
import functools

import jax
import jax.numpy as jnp
from jax import lax
from jax.experimental import pallas as pl
from jax.experimental.pallas import tpu as pltpu
from jax.sharding import PartitionSpec as P

F32 = jnp.float32
CORES = 2
PIECES = 2
ACC_PIECES = 4
TILE = 256

SLOTS = 8
STEPS = 2 * SLOTS


def kernel(
    n, x_hbm, wg_hbm, wu_hbm, wd_hbm, y_ref,
    x_all, wg, wu, wd, hidden, acc, terms, partner_terms, arrived,
    load_sem, ag_send, ag_recv, relay_send, relay_recv, pt_send, pt_recv,
    far_send, far_recv, plain_send, plain_recv, sum_send, sum_recv,
):
    half, depth = x_all.shape[1:]
    me = lax.axis_index("tp")
    right = {"tp": lax.rem(me + CORES, n)}
    left = {"tp": lax.rem(me + n - CORES, n)}
    partner = {"tp": me + 1 - 2 * lax.rem(me, CORES)}
    part = half // PIECES
    spart = half // ACC_PIECES

    def rows(p, size):
        return pl.ds(p * size, size)

    def remote(src, dst, send, recv, device):
        return pltpu.make_async_remote_copy(
            src_ref=src, dst_ref=dst, send_sem=send, recv_sem=recv,
            device_id=device, device_id_type=pl.DeviceIdType.MESH,
        )

    def mine(slot):
        return 2 * slot + 1

    moves = [(0, 2, right), (1, 3, left), (2, 4, right), (3, 5, left), (0, 6, left), (1, 7, right)]

    def gather(m, p):
        src, dst, device = moves[m]
        return remote(
            x_all.at[mine(src), rows(p, part)], x_all.at[mine(dst), rows(p, part)],
            ag_send.at[m, p], ag_recv.at[m, p], device,
        )

    def relay(slot, p):
        return remote(
            x_all.at[mine(slot), rows(p, part)], x_all.at[2 * slot, rows(p, part)],
            relay_send.at[slot, p], relay_recv.at[slot, p], partner,
        )

    def partner_term(slot):
        return remote(
            x_all.at[2 * slot], partner_terms.at[slot], pt_send.at[slot], pt_recv.at[slot], partner
        )

    def far_term(h, p):
        return remote(
            terms.at[2 + h, rows(p, part)], arrived.at[h, rows(p, part)],
            far_send.at[h, p], far_recv.at[h, p], (right, left)[h],
        )

    def plain_term(h, p):
        return remote(
            terms.at[h, rows(p, part)], arrived.at[2 + h, rows(p, part)],
            plain_send.at[h, p], plain_recv.at[h, p], (left, right)[h],
        )

    def sum_term(h, p):
        return remote(
            terms.at[4 + h, rows(p, spart)], arrived.at[4 + h, rows(p, spart)],
            sum_send.at[h, p], sum_recv.at[h, p], (right, left)[h],
        )

    own = [pltpu.make_async_copy(x_hbm.at[rows(h, half)], x_all.at[mine(h)], load_sem.at[h]) for h in range(2)]
    weights = [
        pltpu.make_async_copy(src, dst, load_sem.at[2 + i])
        for i, (src, dst) in enumerate(((wg_hbm, wg), (wu_hbm, wu), (wd_hbm, wd)))
    ]
    for c in own + weights:
        c.start()
    barrier = pltpu.get_barrier_semaphore()
    for device in (right, left, partner):
        pl.semaphore_signal(barrier, inc=1, device_id=device, device_id_type=pl.DeviceIdType.MESH)
    pl.semaphore_wait(barrier, 3)
    for h in range(2):
        own[h].wait()
        for p in range(PIECES):
            gather(h, p).start()
    for h in range(2):
        for p in range(PIECES):
            relay(h, p).start()
    for c in weights:
        c.wait()

    def arrive(slots, p):
        for slot in slots:
            gather(slot - 2, p).wait_recv()
            if slot in (2, 3):
                gather(slot, p).start()
            relay(slot, p).start()

    def relayed(slot):
        for p in range(PIECES):
            relay(slot, p).wait_recv()

    def start_near2():
        for m in (4, 5):
            for p in range(PIECES):
                gather(m, p).start()

    before = {
        0: [lambda: relayed(0)],
        2: [lambda: relayed(1)],
        4: [lambda: arrive((2, 3), 0), lambda: arrive((2, 3), 1), start_near2, lambda: relayed(2)],
        6: [lambda: relayed(3)],
        8: [lambda: arrive((4, 5), 0), lambda: arrive((4, 5), 1), lambda: relayed(4)],
        10: [lambda: relayed(5)],
        12: [lambda: arrive((6, 7), 0), lambda: arrive((6, 7), 1), lambda: relayed(6)],
        14: [lambda: relayed(7)],
    }

    def add_rows(start, size, srcs, dst):
        chunk = 32

        @pl.loop(0, size // chunk)
        def _(i):
            r = pl.ds(pl.multiple_of(start + i * chunk, chunk), chunk)
            total = srcs[0][r, :].astype(F32)
            for s in srcs[1:]:
                total += s[r, :].astype(F32)
            dst[r, :] = total.astype(dst.dtype)

    def finish_far(h):
        partner_term(4 + h).wait_recv()
        for p in range(PIECES):
            add_rows(p * part, part, [acc.at[0], partner_terms.at[4 + h]], terms.at[2 + h])
            far_term(h, p).start()

    def finish_plain(h):
        partner_term(2 + h).wait_recv()
        add_rows(0, half, [acc.at[0], partner_terms.at[2 + h]], terms.at[h])

    def start_plain():
        for h in range(2):
            for p in range(PIECES):
                plain_term(h, p).start()

    after = {
        5: [lambda: finish_plain(0)],
        7: [lambda: finish_plain(1)],
        9: [lambda: finish_far(0)],
        11: [lambda: finish_far(1), start_plain],
    }

    def step(t, carry):
        for at, actions in before.items():

            @pl.when(t == at)
            def _():
                for a in actions:
                    a()

        rows_in = x_all.at[t]
        for c in range(0, hidden.shape[1], TILE):
            cols = pl.ds(c, TILE)
            gate = jnp.dot(rows_in[...], wg[:, cols], preferred_element_type=F32)
            up = jnp.dot(rows_in[...], wu[:, cols], preferred_element_type=F32)
            hidden[:, cols] = (jax.nn.silu(gate) * up).astype(hidden.dtype)
        slot = t // 2
        to = (t % 2) * (jnp.where(slot < 2, slot + 1, 0) + jnp.where(slot > 5, slot - 3, 0))
        for c in range(0, depth, TILE):
            cols = pl.ds(c, TILE)
            acc[to, :, cols] = jnp.dot(hidden[...], wd[:, cols], preferred_element_type=F32)

        @pl.when(t % 2 == 0)
        def _():
            add_rows(0, half, [acc.at[0]], x_all.at[t])
            partner_term(slot).start()

        for at, actions in after.items():

            @pl.when(t == at)
            def _():
                for a in actions:
                    a()

        return carry

    lax.fori_loop(0, STEPS, step, 0)

    for h in range(2):
        partner_term(6 + h).wait_recv()
    for p in range(PIECES):
        for h in range(2):
            far_term(h, p).wait_recv()
            ratio = ACC_PIECES // PIECES
            for q in range(p * ratio, (p + 1) * ratio):
                add_rows(q * spart, spart, [acc.at[3 + h], partner_terms.at[6 + h], arrived.at[h]], terms.at[4 + h])
                sum_term(h, q).start()
    for h in range(2):
        partner_term(h).wait_recv()
        for p in range(PIECES):
            plain_term(h, p).wait_recv()
        add_rows(0, half, [acc.at[1 + h], partner_terms.at[h], arrived.at[2 + h]], acc.at[1 + h])
    for p in range(ACC_PIECES):
        for h in range(2):
            sum_term(h, p).wait_recv()
            add_rows(p * spart, spart, [acc.at[1 + h], arrived.at[4 + h]], y_ref.at[pl.ds(h * half, half)])

    for p in range(ACC_PIECES):
        for h in range(2):
            sum_term(h, p).wait_send()
    for p in range(PIECES):
        for m in range(6):
            gather(m, p).wait_send()
        for slot in range(SLOTS):
            relay(slot, p).wait_send()
        for h in range(2):
            far_term(h, p).wait_send()
            plain_term(h, p).wait_send()
    for slot in range(SLOTS):
        partner_term(slot).wait_send()


def solution(mesh):
    n = mesh.shape["tp"]

    def step(x, w_gate, w_up, w_down):
        rows, depth = x.shape
        width = w_gate.shape[1]
        half = rows // 2
        dma = pltpu.SemaphoreType.DMA
        bf16 = jnp.bfloat16
        return pl.pallas_call(
            functools.partial(kernel, n),
            out_shape=pltpu.VMEM((rows, depth), bf16),
            in_specs=[pl.BlockSpec(memory_space=pl.ANY)] * 4,
            out_specs=pl.BlockSpec(memory_space=pltpu.VMEM),
            scratch_shapes=[
                pltpu.VMEM((STEPS, half, depth), bf16),
                pltpu.VMEM((depth, width), bf16),
                pltpu.VMEM((depth, width), bf16),
                pltpu.VMEM((width, depth), bf16),
                pltpu.VMEM((half, width), bf16),
                pltpu.VMEM((5, half, depth), F32),
                pltpu.VMEM((6, half, depth), bf16),
                pltpu.VMEM((SLOTS, half, depth), bf16),
                pltpu.VMEM((6, half, depth), bf16),
                dma((5,)),
                dma((6, PIECES)),
                dma((6, PIECES)),
                dma((SLOTS, PIECES)),
                dma((SLOTS, PIECES)),
                dma((SLOTS,)),
                dma((SLOTS,)),
                dma((2, PIECES)),
                dma((2, PIECES)),
                dma((2, PIECES)),
                dma((2, PIECES)),
                dma((2, ACC_PIECES)),
                dma((2, ACC_PIECES)),
            ],
            compiler_params=pltpu.CompilerParams(
                collective_id=0, has_side_effects=True, vmem_limit_bytes=61 * 2**20
            ),
        )(x, w_gate, w_up, w_down)

    return jax.shard_map(
        step,
        mesh=mesh,
        in_specs=(P(("dp", "tp"), None), P(None, "tp"), P(None, "tp"), P("tp", None)),
        out_specs=P(("dp", "tp"), None),
        check_vma=False,
    )
```

```python
import functools

import jax
import jax.numpy as jnp
from jax import lax
from jax.experimental import pallas as pl
from jax.experimental.pallas import tpu as pltpu
from jax.sharding import PartitionSpec as P

F32 = jnp.float32
CORES = 2
PIECES = 2
LAST = 32
TILE = 256

SLOTS = 8
STEPS = 2 * SLOTS


def kernel(
    n, x_hbm, wg_hbm, wu_hbm, wd_hbm, y_ref,
    x_all, wg, wu, wd, hidden, acc, terms, partner_terms, arrived,
    own_sem, weight_sem, ring_send, partner_send, near_recv, half_recv, relay_recv, pt_recv,
    far_recv, plain_recv, sum_recv,
):
    half, depth = x_all.shape[1:]
    me = lax.axis_index("tp")
    right = {"tp": lax.rem(me + CORES, n)}
    left = {"tp": lax.rem(me + n - CORES, n)}
    partner = {"tp": me + 1 - 2 * lax.rem(me, CORES)}
    part = half // PIECES
    pieces = [pl.ds(p * part, part) for p in range(PIECES)]
    whole = pl.ds(0, half)
    sums = [(0, part), (part, half - part - LAST), (half - LAST, LAST)]

    def remote(src, dst, send, recv, device):
        return pltpu.make_async_remote_copy(
            src_ref=src, dst_ref=dst, send_sem=send, recv_sem=recv,
            device_id=device, device_id_type=pl.DeviceIdType.MESH,
        )

    def mine(slot):
        return 2 * slot + 1

    moves = [(0, right), (1, left), (2, right), (3, left), (0, left), (1, right)]

    def gather(slot, p=None):
        src, device = moves[slot - 2]
        rows = whole if p is None else pieces[p]
        recv = near_recv.at[slot - 2, p] if slot < 4 else half_recv.at[slot - 4]
        return remote(
            x_all.at[mine(src), rows], x_all.at[mine(slot), rows], ring_send.at[0], recv, device
        )

    def relay(slot, rows=whole):
        return remote(
            x_all.at[mine(slot), rows], x_all.at[2 * slot, rows],
            partner_send.at[0], relay_recv.at[slot % 2], partner,
        )

    def partner_term(slot):
        return remote(
            x_all.at[2 * slot], partner_terms.at[slot], partner_send.at[0], pt_recv.at[slot % 2], partner
        )

    def far_term(h, p):
        return remote(
            terms.at[2 + h, pieces[p]], arrived.at[h, pieces[p]],
            ring_send.at[0], far_recv.at[h, p], (right, left)[h],
        )

    def plain_term(h):
        return remote(
            terms.at[h], arrived.at[2 + h], ring_send.at[0], plain_recv.at[h], (left, right)[h]
        )

    def sum_term(h, p):
        rows = pl.ds(*sums[p])
        return remote(
            terms.at[4 + h, rows], arrived.at[4 + h, rows],
            ring_send.at[0], sum_recv.at[h, p], (right, left)[h],
        )

    own = [pltpu.make_async_copy(x_hbm.at[pl.ds(h * half, half)], x_all.at[mine(h)], own_sem.at[h]) for h in range(2)]
    weights = [
        pltpu.make_async_copy(src, dst, weight_sem.at[i])
        for i, (src, dst) in enumerate(((wg_hbm, wg), (wu_hbm, wu), (wd_hbm, wd)))
    ]
    for c in own:
        c.start()
    barrier = pltpu.get_barrier_semaphore()
    for device in (right, left, partner):
        pl.semaphore_signal(barrier, inc=1, device_id=device, device_id_type=pl.DeviceIdType.MESH)
    pl.semaphore_wait(barrier, 3)
    for h in range(2):
        own[h].wait()
        for p in range(PIECES):
            gather(2 + h, p).start()
    for c in weights:
        c.start()
    for h in range(2):
        relay(h).start()
    for c in weights:
        c.wait()

    def arrive_near(p):
        for slot in (2, 3):
            gather(slot, p).wait_recv()
            gather(slot + 2, p).start()
            relay(slot, pieces[p]).start()

    def arrive_half(slots):
        for slot in slots:
            gather(slot).wait_recv()
            relay(slot).start()

    def relayed(slot):
        relay(slot).wait_recv()

    def start_near2():
        for slot in (6, 7):
            gather(slot).start()

    def own_terms():
        for h in range(2):
            partner_term(h).wait_recv()

    before = {
        0: [lambda: relayed(0)],
        2: [lambda: relayed(1)],
        4: [own_terms, lambda: arrive_near(0), lambda: arrive_near(1), start_near2, lambda: relayed(2)],
        6: [lambda: relayed(3)],
        8: [lambda: arrive_half((4, 5)), lambda: relayed(4)],
        10: [lambda: relayed(5)],
        12: [lambda: arrive_half((6, 7)), lambda: relayed(6)],
        14: [lambda: relayed(7)],
    }

    def add_rows(start, size, srcs, dst):
        chunk = 32

        @pl.loop(0, size // chunk)
        def _(i):
            r = pl.ds(pl.multiple_of(start + i * chunk, chunk), chunk)
            total = srcs[0][r, :].astype(F32)
            for s in srcs[1:]:
                total += s[r, :].astype(F32)
            dst[r, :] = total.astype(dst.dtype)

    def finish_far(h):
        partner_term(4 + h).wait_recv()
        for p in range(PIECES):
            add_rows(p * part, part, [acc.at[0], partner_terms.at[4 + h]], terms.at[2 + h])
            far_term(h, p).start()

    def finish_plain(h):
        partner_term(2 + h).wait_recv()
        add_rows(0, half, [acc.at[0], partner_terms.at[2 + h]], terms.at[h])

    def start_plain():
        for h in range(2):
            plain_term(h).start()

    after = {
        5: [lambda: finish_plain(0)],
        7: [lambda: finish_plain(1)],
        9: [lambda: finish_far(0)],
        11: [lambda: finish_far(1), start_plain],
    }

    def step(t, carry):
        for at, actions in before.items():

            @pl.when(t == at)
            def _():
                for a in actions:
                    a()

        rows_in = x_all.at[t]
        for c in range(0, hidden.shape[1], TILE):
            cols = pl.ds(c, TILE)
            gate = jnp.dot(rows_in[...], wg[:, cols], preferred_element_type=F32)
            up = jnp.dot(rows_in[...], wu[:, cols], preferred_element_type=F32)
            hidden[:, cols] = (jax.nn.silu(gate) * up).astype(hidden.dtype)
        slot = t // 2
        to = (t % 2) * (jnp.where(slot < 2, slot + 1, 0) + jnp.where(slot > 5, slot - 3, 0))
        for c in range(0, depth, TILE):
            cols = pl.ds(c, TILE)
            acc[to, :, cols] = jnp.dot(hidden[...], wd[:, cols], preferred_element_type=F32)

        @pl.when(t % 2 == 0)
        def _():
            add_rows(0, half, [acc.at[0]], x_all.at[t])
            remote(
                x_all.at[t], partner_terms.at[slot], partner_send.at[0], pt_recv.at[slot % 2], partner
            ).start()

        for at, actions in after.items():

            @pl.when(t == at)
            def _():
                for a in actions:
                    a()

        return carry

    lax.fori_loop(0, STEPS, step, 0)

    for h in range(2):
        partner_term(6 + h).wait_recv()
    for p in range(PIECES):
        for h in range(2):
            far_term(h, p).wait_recv()
            for q in ((0,), (1, 2))[p]:
                add_rows(*sums[q], [acc.at[3 + h], partner_terms.at[6 + h], arrived.at[h]], terms.at[4 + h])
                sum_term(h, q).start()
    for h in range(2):
        plain_term(h).wait_recv()
        add_rows(0, half, [acc.at[1 + h], partner_terms.at[h], arrived.at[2 + h]], acc.at[1 + h])
    pltpu.make_async_copy(x_all, x_all, partner_send.at[0]).wait()
    for p in range(len(sums)):
        for h in range(2):
            sum_term(h, p).wait_recv()
            add_rows(*sums[p], [acc.at[1 + h], arrived.at[4 + h]], y_ref.at[pl.ds(h * half, half)])
    sent = x_all.at[pl.ds(0, 12)]
    pltpu.make_async_copy(sent, sent, ring_send.at[0]).wait()


def solution(mesh):
    n = mesh.shape["tp"]

    def step(x, w_gate, w_up, w_down):
        rows, depth = x.shape
        width = w_gate.shape[1]
        half = rows // 2
        dma = pltpu.SemaphoreType.DMA
        bf16 = jnp.bfloat16
        return pl.pallas_call(
            functools.partial(kernel, n),
            out_shape=pltpu.VMEM((rows, depth), bf16),
            in_specs=[pl.BlockSpec(memory_space=pl.ANY)] * 4,
            out_specs=pl.BlockSpec(memory_space=pltpu.VMEM),
            scratch_shapes=[
                pltpu.VMEM((STEPS, half, depth), bf16),
                pltpu.VMEM((depth, width), bf16),
                pltpu.VMEM((depth, width), bf16),
                pltpu.VMEM((width, depth), bf16),
                pltpu.VMEM((half, width), bf16),
                pltpu.VMEM((5, half, depth), F32),
                pltpu.VMEM((6, half, depth), bf16),
                pltpu.VMEM((SLOTS, half, depth), bf16),
                pltpu.VMEM((6, half, depth), bf16),
                dma((2,)),
                dma((3,)),
                dma((1,)),
                dma((1,)),
                dma((2, PIECES)),
                dma((4,)),
                dma((2,)),
                dma((2,)),
                dma((2, PIECES)),
                dma((2,)),
                dma((2, 3)),
            ],
            compiler_params=pltpu.CompilerParams(
                collective_id=0, has_side_effects=True, vmem_limit_bytes=61 * 2**20
            ),
        )(x, w_gate, w_up, w_down)

    return jax.shard_map(
        step,
        mesh=mesh,
        in_specs=(P(("dp", "tp"), None), P(None, "tp"), P(None, "tp"), P("tp", None)),
        out_specs=P(("dp", "tp"), None),
        check_vma=False,
    )
```

```python
import functools

import jax
import jax.numpy as jnp
from jax import lax
from jax.experimental import pallas as pl
from jax.experimental.pallas import tpu as pltpu
from jax.sharding import PartitionSpec as P

F32 = jnp.float32
CORES = 2
PIECES = 2
FIRST = 64
LAST = 32
TILE = 256

SLOTS = 8
STEPS = 2 * SLOTS


def kernel(
    n, x_hbm, wg_hbm, wu_hbm, wd_hbm, y_ref,
    x_all, wg, wu, wd, hidden, acc, terms, partner_terms, arrived,
    own_sem, weight_sem, ring_send, partner_send, near_recv, half_recv, relay_recv, pt_recv,
    sum_recv,
):
    half, depth = x_all.shape[1:]
    me = lax.axis_index("tp")
    right = {"tp": lax.rem(me + CORES, n)}
    left = {"tp": lax.rem(me + n - CORES, n)}
    partner = {"tp": me + 1 - 2 * lax.rem(me, CORES)}
    part = half // PIECES
    pieces = [pl.ds(p * part, part) for p in range(PIECES)]
    near = [(0, FIRST), (FIRST, half - FIRST)]
    whole = pl.ds(0, half)
    sums = [(0, half - LAST), (half - LAST, LAST)]

    def remote(src, dst, send, recv, device):
        return pltpu.make_async_remote_copy(
            src_ref=src, dst_ref=dst, send_sem=send, recv_sem=recv,
            device_id=device, device_id_type=pl.DeviceIdType.MESH,
        )

    def mine(slot):
        return 2 * slot + 1

    moves = [(0, right), (1, left), (2, right), (3, left), (0, left), (1, right)]

    def gather(slot, p=None):
        src, device = moves[slot - 2]
        rows = whole if p is None else pl.ds(*near[p])
        recv = near_recv.at[slot - 2, p] if slot < 4 else half_recv.at[slot - 4]
        return remote(
            x_all.at[mine(src), rows], x_all.at[mine(slot), rows], ring_send.at[0], recv, device
        )

    def relay(slot, rows=whole):
        return remote(
            x_all.at[mine(slot), rows], x_all.at[2 * slot, rows],
            partner_send.at[0], relay_recv.at[slot % 2], partner,
        )

    def partner_term(slot):
        return remote(
            x_all.at[2 * slot], partner_terms.at[slot], partner_send.at[0], pt_recv.at[slot % 2], partner
        )

    def far_term(h, p):
        return remote(
            terms.at[2 + h, pieces[p]], arrived.at[h, pieces[p]],
            ring_send.at[0], near_recv.at[1 - h, p], (right, left)[h],
        )

    def plain_term(h):
        return remote(
            terms.at[h], arrived.at[2 + h], ring_send.at[0], own_sem.at[h, 0], (left, right)[h]
        )

    def sum_term(h, p):
        rows = pl.ds(*sums[p])
        recv = half_recv.at[h] if p == 0 else sum_recv.at[h]
        return remote(
            terms.at[4 + h, rows], arrived.at[4 + h, rows], ring_send.at[0], recv, (right, left)[h]
        )

    own = [
        pltpu.make_async_copy(
            x_hbm.at[pl.ds(h * half + start, size)], x_all.at[mine(h), pl.ds(start, size)], own_sem.at[h, p]
        )
        for p, (start, size) in enumerate(near)
        for h in range(2)
    ]
    weights = [
        pltpu.make_async_copy(src, dst, weight_sem.at[0])
        for src, dst in ((wg_hbm, wg), (wu_hbm, wu), (wd_hbm, wd))
    ]
    for c in own:
        c.start()
    barrier = pltpu.get_barrier_semaphore()
    for device in (right, left, partner):
        pl.semaphore_signal(barrier, inc=1, device_id=device, device_id_type=pl.DeviceIdType.MESH)
    pl.semaphore_wait(barrier, 3)
    for p in range(len(near)):
        for h in range(2):
            own[2 * p + h].wait()
            gather(2 + h, p).start()
    for c in weights:
        c.start()
    for h in range(2):
        relay(h).start()
    blocks = 3 * wg.shape[1] // half
    assert wd.shape == wg.shape[::-1] and blocks <= STEPS
    loaded = x_all.at[pl.ds(0, blocks)]
    pltpu.make_async_copy(loaded, loaded, weight_sem.at[0]).wait()

    def arrive_near(p):
        for slot in (2, 3):
            gather(slot, p).wait_recv()
            gather(slot + 2, p).start()
            relay(slot, pl.ds(*near[p])).start()

    def arrive_half(slots):
        for slot in slots:
            gather(slot).wait_recv()
            relay(slot).start()

    def relayed(slot):
        relay(slot).wait_recv()

    def start_near2():
        for slot in (6, 7):
            gather(slot).start()

    def own_terms():
        for h in range(2):
            partner_term(h).wait_recv()

    before = {
        0: [lambda: relayed(0)],
        2: [lambda: relayed(1)],
        4: [own_terms, lambda: arrive_near(0), lambda: arrive_near(1), start_near2, lambda: relayed(2)],
        6: [lambda: relayed(3)],
        8: [lambda: arrive_half((4, 5)), lambda: relayed(4)],
        10: [lambda: relayed(5)],
        12: [lambda: arrive_half((6, 7)), lambda: relayed(6)],
        14: [lambda: relayed(7)],
    }

    def add_rows(start, size, srcs, dst):
        chunk = 32

        @pl.loop(0, size // chunk)
        def _(i):
            r = pl.ds(pl.multiple_of(start + i * chunk, chunk), chunk)
            total = srcs[0][r, :].astype(F32)
            for s in srcs[1:]:
                total += s[r, :].astype(F32)
            dst[r, :] = total.astype(dst.dtype)

    def finish_far(h):
        partner_term(4 + h).wait_recv()
        for p in range(PIECES):
            add_rows(p * part, part, [acc.at[0], partner_terms.at[4 + h]], terms.at[2 + h])
            far_term(h, p).start()

    def finish_plain(h):
        partner_term(2 + h).wait_recv()
        add_rows(0, half, [acc.at[0], partner_terms.at[2 + h]], terms.at[h])

    def start_plain():
        for h in range(2):
            plain_term(h).start()

    after = {
        5: [lambda: finish_plain(0)],
        7: [lambda: finish_plain(1)],
        9: [lambda: finish_far(0)],
        11: [lambda: finish_far(1), start_plain],
    }

    def step(t, carry):
        for at, actions in before.items():

            @pl.when(t == at)
            def _():
                for a in actions:
                    a()

        rows_in = x_all.at[t]
        for c in range(0, hidden.shape[1], TILE):
            cols = pl.ds(c, TILE)
            gate = jnp.dot(rows_in[...], wg[:, cols], preferred_element_type=F32)
            up = jnp.dot(rows_in[...], wu[:, cols], preferred_element_type=F32)
            hidden[:, cols] = (jax.nn.silu(gate) * up).astype(hidden.dtype)
        slot = t // 2
        to = (t % 2) * (jnp.where(slot < 2, slot + 1, 0) + jnp.where(slot > 5, slot - 3, 0))
        for c in range(0, depth, TILE):
            cols = pl.ds(c, TILE)
            acc[to, :, cols] = jnp.dot(hidden[...], wd[:, cols], preferred_element_type=F32)

        @pl.when(t % 2 == 0)
        def _():
            add_rows(0, half, [acc.at[0]], x_all.at[t])
            remote(
                x_all.at[t], partner_terms.at[slot], partner_send.at[0], pt_recv.at[slot % 2], partner
            ).start()

        for at, actions in after.items():

            @pl.when(t == at)
            def _():
                for a in actions:
                    a()

        return carry

    lax.fori_loop(0, STEPS, step, 0)

    for h in range(2):
        partner_term(6 + h).wait_recv()
    for p in range(PIECES):
        for h in range(2):
            far_term(h, p).wait_recv()
    for q in range(len(sums)):
        for h in range(2):
            add_rows(*sums[q], [acc.at[3 + h], partner_terms.at[6 + h], arrived.at[h]], terms.at[4 + h])
            sum_term(h, q).start()
    for h in range(2):
        plain_term(h).wait_recv()
        add_rows(0, half, [acc.at[1 + h], partner_terms.at[h], arrived.at[2 + h]], acc.at[1 + h])
    pltpu.make_async_copy(x_all, x_all, partner_send.at[0]).wait()
    for p in range(len(sums)):
        for h in range(2):
            sum_term(h, p).wait_recv()
            add_rows(*sums[p], [acc.at[1 + h], arrived.at[4 + h]], y_ref.at[pl.ds(h * half, half)])
    sent = x_all.at[pl.ds(0, 12)]
    pltpu.make_async_copy(sent, sent, ring_send.at[0]).wait()


def solution(mesh):
    n = mesh.shape["tp"]

    def step(x, w_gate, w_up, w_down):
        rows, depth = x.shape
        width = w_gate.shape[1]
        half = rows // 2
        dma = pltpu.SemaphoreType.DMA
        bf16 = jnp.bfloat16
        return pl.pallas_call(
            functools.partial(kernel, n),
            out_shape=pltpu.VMEM((rows, depth), bf16),
            in_specs=[pl.BlockSpec(memory_space=pl.ANY)] * 4,
            out_specs=pl.BlockSpec(memory_space=pltpu.VMEM),
            scratch_shapes=[
                pltpu.VMEM((STEPS, half, depth), bf16),
                pltpu.VMEM((depth, width), bf16),
                pltpu.VMEM((depth, width), bf16),
                pltpu.VMEM((width, depth), bf16),
                pltpu.VMEM((half, width), bf16),
                pltpu.VMEM((5, half, depth), F32),
                pltpu.VMEM((6, half, depth), bf16),
                pltpu.VMEM((SLOTS, half, depth), bf16),
                pltpu.VMEM((6, half, depth), bf16),
                dma((2, 2)),
                dma((1,)),
                dma((1,)),
                dma((1,)),
                dma((2, PIECES)),
                dma((4,)),
                dma((2,)),
                dma((2,)),
                dma((2,)),
            ],
            compiler_params=pltpu.CompilerParams(
                collective_id=0, has_side_effects=True, vmem_limit_bytes=61 * 2**20
            ),
        )(x, w_gate, w_up, w_down)

    return jax.shard_map(
        step,
        mesh=mesh,
        in_specs=(P(("dp", "tp"), None), P(None, "tp"), P(None, "tp"), P("tp", None)),
        out_specs=P(("dp", "tp"), None),
        check_vma=False,
    )
```

```python
import functools

import jax
import jax.numpy as jnp
from jax import lax
from jax.experimental import pallas as pl
from jax.experimental.pallas import tpu as pltpu
from jax.sharding import PartitionSpec as P

F32 = jnp.float32
CORES = 2
PIECES = 2
FIRST = 32
LAST = 32
TILE = 256

SLOTS = 8
STEPS = 2 * SLOTS


def kernel(
    n, x_hbm, wg_hbm, wu_hbm, wd_hbm, y_ref,
    x_all, wg, wu, wd, hidden, acc, terms, partner_terms, arrived,
    own_sem, weight_sem, ring_send, partner_send, near_recv, half_recv, relay_recv, pt_recv,
):
    half, depth = x_all.shape[1:]
    me = lax.axis_index("tp")
    right = {"tp": lax.rem(me + CORES, n)}
    left = {"tp": lax.rem(me + n - CORES, n)}
    partner = {"tp": me + 1 - 2 * lax.rem(me, CORES)}
    part = half // PIECES
    pieces = [pl.ds(p * part, part) for p in range(PIECES)]
    near = [(0, FIRST), (FIRST, half - FIRST)]
    whole = pl.ds(0, half)
    sums = [(0, half - LAST), (half - LAST, LAST)]

    def remote(src, dst, send, recv, device):
        return pltpu.make_async_remote_copy(
            src_ref=src, dst_ref=dst, send_sem=send, recv_sem=recv,
            device_id=device, device_id_type=pl.DeviceIdType.MESH,
        )

    def mine(slot):
        return 2 * slot + 1

    moves = [(0, right), (1, left), (2, right), (3, left), (0, left), (1, right)]

    def gather(slot, p=None):
        src, device = moves[slot - 2]
        rows = whole if p is None else pl.ds(*near[p])
        recv = near_recv.at[slot - 2, p] if slot < 4 else half_recv.at[slot - 4] if slot < 6 else own_sem.at[slot - 6, 0]
        return remote(
            x_all.at[mine(src), rows], x_all.at[mine(slot), rows], ring_send.at[0], recv, device
        )

    def relay(slot, rows=whole):
        return remote(
            x_all.at[mine(slot), rows], x_all.at[2 * slot, rows],
            partner_send.at[0], relay_recv.at[slot % 2], partner,
        )

    def partner_term(slot):
        return remote(
            x_all.at[2 * slot], partner_terms.at[slot], partner_send.at[0], pt_recv.at[slot % 2], partner
        )

    def far_term(h, rows=whole):
        return remote(
            terms.at[2 + h, rows], arrived.at[h, rows], ring_send.at[0], near_recv.at[1 - h, 0], (right, left)[h]
        )

    def plain_term(h):
        return remote(
            terms.at[h], arrived.at[2 + h], ring_send.at[0], near_recv.at[h, 1], (left, right)[h]
        )

    def sum_term(h, p):
        rows = pl.ds(*sums[p])
        recv = half_recv.at[h] if p == 0 else own_sem.at[h, 1]
        return remote(
            terms.at[4 + h, rows], arrived.at[4 + h, rows], ring_send.at[0], recv, (right, left)[h]
        )

    own = [
        pltpu.make_async_copy(
            x_hbm.at[pl.ds(h * half + start, size)], x_all.at[mine(h), pl.ds(start, size)], own_sem.at[h, p]
        )
        for p, (start, size) in enumerate(near)
        for h in range(2)
    ]
    weights = [
        pltpu.make_async_copy(src, dst, weight_sem.at[0])
        for src, dst in ((wg_hbm, wg), (wu_hbm, wu), (wd_hbm, wd))
    ]
    for c in own + weights:
        c.start()
    barrier = pltpu.get_barrier_semaphore()
    for device in (right, left, partner):
        pl.semaphore_signal(barrier, inc=1, device_id=device, device_id_type=pl.DeviceIdType.MESH)
    pl.semaphore_wait(barrier, 3)
    for p in range(len(near)):
        for h in range(2):
            own[2 * p + h].wait()
            gather(2 + h, p).start()
    for h in range(2):
        relay(h).start()
    def arrive_near(p):
        for slot in (2, 3):
            gather(slot, p).wait_recv()
            gather(slot + 2, p).start()
            relay(slot, pl.ds(*near[p])).start()

    def arrive_half(slots):
        for slot in slots:
            gather(slot).wait_recv()
            relay(slot).start()

    blocks = 3 * wg.shape[1] // half
    assert wd.shape == wg.shape[::-1] and blocks <= STEPS
    loaded = x_all.at[pl.ds(0, blocks)]

    def have_weights():
        pltpu.make_async_copy(loaded, loaded, weight_sem.at[0]).wait()

    def relayed(slot):
        relay(slot).wait_recv()

    def start_near2():
        for slot in (6, 7):
            gather(slot).start()

    def own_terms():
        for h in range(2):
            partner_term(h).wait_recv()

    before = {
        0: [lambda: relayed(0), have_weights],
        2: [lambda: relayed(1)],
        4: [own_terms, lambda: arrive_near(0), lambda: arrive_near(1), start_near2, lambda: relayed(2)],
        6: [lambda: relayed(3)],
        8: [lambda: arrive_half((4, 5)), lambda: relayed(4)],
        10: [lambda: relayed(5)],
        12: [lambda: arrive_half((6, 7)), lambda: relayed(6)],
        14: [lambda: relayed(7)],
    }

    def add_rows(start, size, srcs, dst):
        chunk = 32

        @pl.loop(0, size // chunk)
        def _(i):
            r = pl.ds(pl.multiple_of(start + i * chunk, chunk), chunk)
            total = srcs[0][r, :].astype(F32)
            for s in srcs[1:]:
                total += s[r, :].astype(F32)
            dst[r, :] = total.astype(dst.dtype)

    def finish_far(h):
        partner_term(4 + h).wait_recv()
        for p in range(PIECES):
            add_rows(p * part, part, [acc.at[0], partner_terms.at[4 + h]], terms.at[2 + h])
            far_term(h, pieces[p]).start()

    def finish_plain(h):
        partner_term(2 + h).wait_recv()
        add_rows(0, half, [acc.at[0], partner_terms.at[2 + h]], terms.at[h])

    def start_plain():
        for h in range(2):
            plain_term(h).start()

    after = {
        5: [lambda: finish_plain(0)],
        7: [lambda: finish_plain(1)],
        9: [lambda: finish_far(0)],
        11: [lambda: finish_far(1), start_plain],
    }

    def step(t, carry):
        for at, actions in before.items():

            @pl.when(t == at)
            def _():
                for a in actions:
                    a()

        rows_in = x_all.at[t]
        for c in range(0, hidden.shape[1], TILE):
            cols = pl.ds(c, TILE)
            gate = jnp.dot(rows_in[...], wg[:, cols], preferred_element_type=F32)
            up = jnp.dot(rows_in[...], wu[:, cols], preferred_element_type=F32)
            hidden[:, cols] = (jax.nn.silu(gate) * up).astype(hidden.dtype)
        slot = t // 2
        to = (t % 2) * (jnp.where(slot < 2, slot + 1, 0) + jnp.where(slot > 5, slot - 3, 0))
        for c in range(0, depth, TILE):
            cols = pl.ds(c, TILE)
            acc[to, :, cols] = jnp.dot(hidden[...], wd[:, cols], preferred_element_type=F32)

        @pl.when(t % 2 == 0)
        def _():
            add_rows(0, half, [acc.at[0]], x_all.at[t])
            remote(
                x_all.at[t], partner_terms.at[slot], partner_send.at[0], pt_recv.at[slot % 2], partner
            ).start()

        for at, actions in after.items():

            @pl.when(t == at)
            def _():
                for a in actions:
                    a()

        return carry

    lax.fori_loop(0, STEPS, step, 0)

    for h in range(2):
        partner_term(6 + h).wait_recv()
    for h in range(2):
        far_term(h).wait_recv()
    for q in range(len(sums)):
        for h in range(2):
            add_rows(*sums[q], [acc.at[3 + h], partner_terms.at[6 + h], arrived.at[h]], terms.at[4 + h])
            sum_term(h, q).start()
    for h in range(2):
        plain_term(h).wait_recv()
        add_rows(0, half, [acc.at[1 + h], partner_terms.at[h], arrived.at[2 + h]], acc.at[1 + h])
    pltpu.make_async_copy(x_all, x_all, partner_send.at[0]).wait()
    for p in range(len(sums)):
        for h in range(2):
            sum_term(h, p).wait_recv()
            add_rows(*sums[p], [acc.at[1 + h], arrived.at[4 + h]], y_ref.at[pl.ds(h * half, half)])
    sent = x_all.at[pl.ds(0, 12)]
    pltpu.make_async_copy(sent, sent, ring_send.at[0]).wait()


def solution(mesh):
    n = mesh.shape["tp"]

    def step(x, w_gate, w_up, w_down):
        rows, depth = x.shape
        width = w_gate.shape[1]
        half = rows // 2
        dma = pltpu.SemaphoreType.DMA
        bf16 = jnp.bfloat16
        return pl.pallas_call(
            functools.partial(kernel, n),
            out_shape=pltpu.VMEM((rows, depth), bf16),
            in_specs=[pl.BlockSpec(memory_space=pl.ANY)] * 4,
            out_specs=pl.BlockSpec(memory_space=pltpu.VMEM),
            scratch_shapes=[
                pltpu.VMEM((STEPS, half, depth), bf16),
                pltpu.VMEM((depth, width), bf16),
                pltpu.VMEM((depth, width), bf16),
                pltpu.VMEM((width, depth), bf16),
                pltpu.VMEM((half, width), bf16),
                pltpu.VMEM((5, half, depth), F32),
                pltpu.VMEM((6, half, depth), bf16),
                pltpu.VMEM((SLOTS, half, depth), bf16),
                pltpu.VMEM((6, half, depth), bf16),
                dma((2, 2)),
                dma((1,)),
                dma((1,)),
                dma((1,)),
                dma((2, PIECES)),
                dma((2,)),
                dma((2,)),
                dma((2,)),
            ],
            compiler_params=pltpu.CompilerParams(
                collective_id=0, has_side_effects=True, vmem_limit_bytes=61 * 2**20
            ),
        )(x, w_gate, w_up, w_down)

    return jax.shard_map(
        step,
        mesh=mesh,
        in_specs=(P(("dp", "tp"), None), P(None, "tp"), P(None, "tp"), P("tp", None)),
        out_specs=P(("dp", "tp"), None),
        check_vma=False,
    )
```

```python
import functools

import jax
import jax.numpy as jnp
from jax import lax
from jax.experimental import pallas as pl
from jax.experimental.pallas import tpu as pltpu
from jax.sharding import PartitionSpec as P

F32 = jnp.float32
CORES = 2
PIECES = 2
FIRST = 64
LAST = 32
TILE = 256

SLOTS = 8
STEPS = 2 * SLOTS


def kernel(
    n, x_hbm, wg_hbm, wu_hbm, wd_hbm, y_ref,
    x_all, wg, wu, wd, hidden, acc, terms, partner_terms, arrived,
    own_sem, weight_sem, ring_send, partner_send, near_recv, half_recv, relay_recv, pt_recv,
):
    half, depth = x_all.shape[1:]
    me = lax.axis_index("tp")
    right = {"tp": lax.rem(me + CORES, n)}
    left = {"tp": lax.rem(me + n - CORES, n)}
    partner = {"tp": me + 1 - 2 * lax.rem(me, CORES)}
    part = half // PIECES
    pieces = [pl.ds(p * part, part) for p in range(PIECES)]
    near = [(0, FIRST), (FIRST, half - FIRST)]
    whole = pl.ds(0, half)
    sums = [(0, half - LAST), (half - LAST, LAST)]

    def remote(src, dst, send, recv, device):
        return pltpu.make_async_remote_copy(
            src_ref=src, dst_ref=dst, send_sem=send, recv_sem=recv,
            device_id=device, device_id_type=pl.DeviceIdType.MESH,
        )

    def mine(slot):
        return 2 * slot + 1

    moves = [(0, right), (1, left), (2, right), (3, left), (0, left), (1, right)]

    def gather(slot, p=None, start=None):
        src, device = moves[slot - 2]
        rows = whole if p is None else pl.ds(*near[p])
        recv = near_recv.at[slot - 2, p] if slot < 4 else half_recv.at[slot - 4] if slot < 6 else own_sem.at[slot - 6, 0]
        origin = x_all.at[mine(src), rows] if start is None else start
        return remote(origin, x_all.at[mine(slot), rows], ring_send.at[0], recv, device)

    def relay(slot, rows=whole):
        return remote(
            x_all.at[mine(slot), rows], x_all.at[2 * slot, rows],
            partner_send.at[0], relay_recv.at[slot % 2], partner,
        )

    def partner_term(slot):
        return remote(
            x_all.at[2 * slot], partner_terms.at[slot], partner_send.at[0], pt_recv.at[slot % 2], partner
        )

    def far_term(h, rows=whole):
        return remote(
            terms.at[2 + h, rows], arrived.at[h, rows], ring_send.at[0], near_recv.at[1 - h, 0], (right, left)[h]
        )

    def plain_term(h):
        return remote(
            terms.at[h], arrived.at[2 + h], ring_send.at[0], near_recv.at[h, 1], (left, right)[h]
        )

    def sum_term(h, p):
        rows = pl.ds(*sums[p])
        recv = half_recv.at[h] if p == 0 else own_sem.at[h, 1]
        return remote(
            terms.at[4 + h, rows], arrived.at[4 + h, rows], ring_send.at[0], recv, (right, left)[h]
        )

    own = [
        pltpu.make_async_copy(
            x_hbm.at[pl.ds(h * half + start, size)], x_all.at[mine(h), pl.ds(start, size)], own_sem.at[h, p]
        )
        for p, (start, size) in enumerate(near)
        for h in range(2)
    ]
    weights = [
        pltpu.make_async_copy(src, dst, weight_sem.at[0])
        for src, dst in ((wg_hbm, wg), (wu_hbm, wu), (wd_hbm, wd))
    ]
    barrier = pltpu.get_barrier_semaphore()
    for device in (partner, right, left):
        pl.semaphore_signal(barrier, inc=1, device_id=device, device_id_type=pl.DeviceIdType.MESH)
    for c in own + weights:
        c.start()
    pl.semaphore_wait(barrier, 3)
    for h in range(2):
        gather(2 + h, 0, x_hbm.at[pl.ds(h * half, FIRST)]).start()
    for h in range(2):
        own[h].wait()
    for h in range(2):
        own[2 + h].wait()
        gather(2 + h, 1).start()
    for h in range(2):
        relay(h).start()
    def arrive_near(p):
        for slot in (2, 3):
            gather(slot, p).wait_recv()
            gather(slot + 2, p).start()
            relay(slot, pl.ds(*near[p])).start()

    def arrive_half(slots):
        for slot in slots:
            gather(slot).wait_recv()
            relay(slot).start()

    blocks = 3 * wg.shape[1] // half
    assert wd.shape == wg.shape[::-1] and blocks <= STEPS
    loaded = x_all.at[pl.ds(0, blocks)]

    def have_weights():
        pltpu.make_async_copy(loaded, loaded, weight_sem.at[0]).wait()

    def relayed(slot):
        relay(slot).wait_recv()

    def start_near2():
        for slot in (6, 7):
            gather(slot).start()

    def own_terms():
        for h in range(2):
            partner_term(h).wait_recv()

    before = {
        0: [lambda: relayed(0), have_weights],
        2: [lambda: relayed(1)],
        4: [own_terms, lambda: arrive_near(0), lambda: arrive_near(1), start_near2, lambda: relayed(2)],
        6: [lambda: relayed(3)],
        8: [lambda: arrive_half((4, 5)), lambda: relayed(4)],
        10: [lambda: relayed(5)],
        12: [lambda: arrive_half((6, 7)), lambda: relayed(6)],
        14: [lambda: relayed(7)],
    }

    def add_rows(start, size, srcs, dst):
        chunk = 32

        @pl.loop(0, size // chunk)
        def _(i):
            r = pl.ds(pl.multiple_of(start + i * chunk, chunk), chunk)
            total = srcs[0][r, :].astype(F32)
            for s in srcs[1:]:
                total += s[r, :].astype(F32)
            dst[r, :] = total.astype(dst.dtype)

    def finish_far(h):
        partner_term(4 + h).wait_recv()
        for p in range(PIECES):
            add_rows(p * part, part, [acc.at[0], partner_terms.at[4 + h]], terms.at[2 + h])
            far_term(h, pieces[p]).start()

    def finish_plain(h):
        partner_term(2 + h).wait_recv()
        add_rows(0, half, [acc.at[0], partner_terms.at[2 + h]], terms.at[h])

    def start_plain():
        for h in range(2):
            plain_term(h).start()

    after = {
        5: [lambda: finish_plain(0)],
        7: [lambda: finish_plain(1)],
        9: [lambda: finish_far(0)],
        11: [lambda: finish_far(1), start_plain],
    }

    def step(t, carry):
        for at, actions in before.items():

            @pl.when(t == at)
            def _():
                for a in actions:
                    a()

        rows_in = x_all.at[t]
        for c in range(0, hidden.shape[1], TILE):
            cols = pl.ds(c, TILE)
            gate = jnp.dot(rows_in[...], wg[:, cols], preferred_element_type=F32)
            up = jnp.dot(rows_in[...], wu[:, cols], preferred_element_type=F32)
            hidden[:, cols] = (jax.nn.silu(gate) * up).astype(hidden.dtype)
        slot = t // 2
        to = (t % 2) * (jnp.where(slot < 2, slot + 1, 0) + jnp.where(slot > 5, slot - 3, 0))
        for c in range(0, depth, TILE):
            cols = pl.ds(c, TILE)
            acc[to, :, cols] = jnp.dot(hidden[...], wd[:, cols], preferred_element_type=F32)

        @pl.when(t % 2 == 0)
        def _():
            add_rows(0, half, [acc.at[0]], x_all.at[t])
            remote(
                x_all.at[t], partner_terms.at[slot], partner_send.at[0], pt_recv.at[slot % 2], partner
            ).start()

        for at, actions in after.items():

            @pl.when(t == at)
            def _():
                for a in actions:
                    a()

        return carry

    lax.fori_loop(0, STEPS, step, 0)

    for h in range(2):
        partner_term(6 + h).wait_recv()
    for h in range(2):
        far_term(h).wait_recv()
    for q in range(len(sums)):
        for h in range(2):
            add_rows(*sums[q], [acc.at[3 + h], partner_terms.at[6 + h], arrived.at[h]], terms.at[4 + h])
            sum_term(h, q).start()
    for h in range(2):
        plain_term(h).wait_recv()
        add_rows(0, half, [acc.at[1 + h], partner_terms.at[h], arrived.at[2 + h]], acc.at[1 + h])
    pltpu.make_async_copy(x_all, x_all, partner_send.at[0]).wait()
    for p in range(len(sums)):
        for h in range(2):
            sum_term(h, p).wait_recv()
            add_rows(*sums[p], [acc.at[1 + h], arrived.at[4 + h]], y_ref.at[pl.ds(h * half, half)])
    sent = x_all.at[pl.ds(0, 12)]
    pltpu.make_async_copy(sent, sent, ring_send.at[0]).wait()


def solution(mesh):
    n = mesh.shape["tp"]

    def step(x, w_gate, w_up, w_down):
        rows, depth = x.shape
        width = w_gate.shape[1]
        half = rows // 2
        dma = pltpu.SemaphoreType.DMA
        bf16 = jnp.bfloat16
        return pl.pallas_call(
            functools.partial(kernel, n),
            out_shape=pltpu.VMEM((rows, depth), bf16),
            in_specs=[pl.BlockSpec(memory_space=pl.ANY)] * 4,
            out_specs=pl.BlockSpec(memory_space=pltpu.VMEM),
            scratch_shapes=[
                pltpu.VMEM((STEPS, half, depth), bf16),
                pltpu.VMEM((depth, width), bf16),
                pltpu.VMEM((depth, width), bf16),
                pltpu.VMEM((width, depth), bf16),
                pltpu.VMEM((half, width), bf16),
                pltpu.VMEM((5, half, depth), F32),
                pltpu.VMEM((6, half, depth), bf16),
                pltpu.VMEM((SLOTS, half, depth), bf16),
                pltpu.VMEM((6, half, depth), bf16),
                dma((2, 2)),
                dma((1,)),
                dma((1,)),
                dma((1,)),
                dma((2, PIECES)),
                dma((2,)),
                dma((2,)),
                dma((2,)),
            ],
            compiler_params=pltpu.CompilerParams(
                collective_id=0, has_side_effects=True, vmem_limit_bytes=61 * 2**20
            ),
        )(x, w_gate, w_up, w_down)

    return jax.shard_map(
        step,
        mesh=mesh,
        in_specs=(P(("dp", "tp"), None), P(None, "tp"), P(None, "tp"), P("tp", None)),
        out_specs=P(("dp", "tp"), None),
        check_vma=False,
    )
```

```python
import functools

import jax
import jax.numpy as jnp
from jax import lax
from jax.experimental import pallas as pl
from jax.experimental.pallas import tpu as pltpu
from jax.sharding import PartitionSpec as P

F32 = jnp.float32
CORES = 2
PIECES = 2
FIRST = 64
LAST = 32
TILE = 256

SLOTS = 8
STEPS = 2 * SLOTS


def kernel(
    n, x_hbm, wg_hbm, wu_hbm, wd_hbm, y_ref,
    x_all, wg, wu, wd, hidden, acc, terms, partner_terms, arrived,
    own_sem, weight_sem, ring_send, partner_send, near_recv, half_recv, relay_recv, pt_recv,
):
    half, depth = x_all.shape[1:]
    me = lax.axis_index("tp")
    right = {"tp": lax.rem(me + CORES, n)}
    left = {"tp": lax.rem(me + n - CORES, n)}
    partner = {"tp": me + 1 - 2 * lax.rem(me, CORES)}
    part = half // PIECES
    pieces = [pl.ds(p * part, part) for p in range(PIECES)]
    near = [(0, FIRST), (FIRST, half - FIRST)]
    whole = pl.ds(0, half)
    sums = [(0, half - LAST), (half - LAST, LAST)]

    def remote(src, dst, send, recv, device):
        return pltpu.make_async_remote_copy(
            src_ref=src, dst_ref=dst, send_sem=send, recv_sem=recv,
            device_id=device, device_id_type=pl.DeviceIdType.MESH,
        )

    def mine(slot):
        return 2 * slot + 1

    moves = [(0, right), (1, left), (2, right), (3, left), (0, left), (1, right)]

    def gather(slot, p=None, start=None):
        src, device = moves[slot - 2]
        rows = whole if p is None else pl.ds(*near[p])
        recv = near_recv.at[slot - 2, p] if slot < 4 else half_recv.at[slot - 4] if slot < 6 else own_sem.at[slot - 6, 0]
        origin = x_all.at[mine(src), rows] if start is None else start
        return remote(origin, x_all.at[mine(slot), rows], ring_send.at[0], recv, device)

    def relay(slot, rows=whole):
        return remote(
            x_all.at[mine(slot), rows], x_all.at[2 * slot, rows],
            partner_send.at[0], relay_recv.at[slot % 2], partner,
        )

    def partner_term(slot):
        return remote(
            x_all.at[2 * slot], partner_terms.at[slot], partner_send.at[0], pt_recv.at[slot % 2], partner
        )

    def far_term(h, rows=whole):
        return remote(
            terms.at[2 + h, rows], arrived.at[h, rows], ring_send.at[0], near_recv.at[1 - h, 0], (right, left)[h]
        )

    def plain_term(h):
        return remote(
            terms.at[h], arrived.at[2 + h], ring_send.at[0], near_recv.at[h, 1], (left, right)[h]
        )

    def sum_term(h, p):
        rows = pl.ds(*sums[p])
        recv = half_recv.at[h] if p == 0 else own_sem.at[h, 1]
        return remote(
            terms.at[4 + h, rows], arrived.at[4 + h, rows], ring_send.at[0], recv, (right, left)[h]
        )

    own = [
        pltpu.make_async_copy(
            x_hbm.at[pl.ds(h * half + start, size)], x_all.at[mine(h), pl.ds(start, size)], own_sem.at[h, p]
        )
        for p, (start, size) in enumerate(near)
        for h in range(2)
    ]
    weights = [
        pltpu.make_async_copy(src, dst, weight_sem.at[0])
        for src, dst in ((wg_hbm, wg), (wu_hbm, wu), (wd_hbm, wd))
    ]
    barrier = pltpu.get_barrier_semaphore()

    def greet(device):
        pl.semaphore_signal(barrier, inc=1, device_id=device, device_id_type=pl.DeviceIdType.MESH)

    core = lax.rem(me, CORES)
    greet(right)
    greet(left)
    for c in own + weights:
        c.start()
    pl.semaphore_wait(barrier, 3 - core)
    greet(partner)
    for h in range(2):
        gather(2 + h, 0, x_hbm.at[pl.ds(h * half, FIRST)]).start()
    for h in range(2):
        own[h].wait()
    for h in range(2):
        own[2 + h].wait()
        gather(2 + h, 1).start()

    @pl.when(core == 1)
    def _():
        pl.semaphore_wait(barrier, 1)

    for h in range(2):
        relay(h).start()
    def arrive_near(p):
        for slot in (2, 3):
            gather(slot, p).wait_recv()
            gather(slot + 2, p).start()
            relay(slot, pl.ds(*near[p])).start()

    def arrive_half(slots):
        for slot in slots:
            gather(slot).wait_recv()
            relay(slot).start()

    blocks = 3 * wg.shape[1] // half
    assert wd.shape == wg.shape[::-1] and blocks <= STEPS
    loaded = x_all.at[pl.ds(0, blocks)]

    def have_weights():
        pltpu.make_async_copy(loaded, loaded, weight_sem.at[0]).wait()

    def relayed(slot):
        relay(slot).wait_recv()

    def start_near2():
        for slot in (6, 7):
            gather(slot).start()

    def own_terms():
        for h in range(2):
            partner_term(h).wait_recv()

    before = {
        0: [lambda: relayed(0), have_weights],
        2: [lambda: relayed(1)],
        4: [own_terms, lambda: arrive_near(0), lambda: arrive_near(1), start_near2, lambda: relayed(2)],
        6: [lambda: relayed(3)],
        8: [lambda: arrive_half((4, 5)), lambda: relayed(4)],
        10: [lambda: relayed(5)],
        12: [lambda: arrive_half((6, 7)), lambda: relayed(6)],
        14: [lambda: relayed(7)],
    }

    def add_rows(start, size, srcs, dst):
        chunk = 32

        @pl.loop(0, size // chunk)
        def _(i):
            r = pl.ds(pl.multiple_of(start + i * chunk, chunk), chunk)
            total = srcs[0][r, :].astype(F32)
            for s in srcs[1:]:
                total += s[r, :].astype(F32)
            dst[r, :] = total.astype(dst.dtype)

    def finish_far(h):
        partner_term(4 + h).wait_recv()
        for p in range(PIECES):
            add_rows(p * part, part, [acc.at[0], partner_terms.at[4 + h]], terms.at[2 + h])
            far_term(h, pieces[p]).start()

    def finish_plain(h):
        partner_term(2 + h).wait_recv()
        add_rows(0, half, [acc.at[0], partner_terms.at[2 + h]], terms.at[h])

    def start_plain():
        for h in range(2):
            plain_term(h).start()

    after = {
        5: [lambda: finish_plain(0)],
        7: [lambda: finish_plain(1)],
        9: [lambda: finish_far(0)],
        11: [lambda: finish_far(1), start_plain],
    }

    def step(t, carry):
        for at, actions in before.items():

            @pl.when(t == at)
            def _():
                for a in actions:
                    a()

        rows_in = x_all.at[t]
        for c in range(0, hidden.shape[1], TILE):
            cols = pl.ds(c, TILE)
            gate = jnp.dot(rows_in[...], wg[:, cols], preferred_element_type=F32)
            up = jnp.dot(rows_in[...], wu[:, cols], preferred_element_type=F32)
            hidden[:, cols] = (jax.nn.silu(gate) * up).astype(hidden.dtype)
        slot = t // 2
        to = (t % 2) * (jnp.where(slot < 2, slot + 1, 0) + jnp.where(slot > 5, slot - 3, 0))
        for c in range(0, depth, TILE):
            cols = pl.ds(c, TILE)
            acc[to, :, cols] = jnp.dot(hidden[...], wd[:, cols], preferred_element_type=F32)

        @pl.when(t % 2 == 0)
        def _():
            add_rows(0, half, [acc.at[0]], x_all.at[t])
            remote(
                x_all.at[t], partner_terms.at[slot], partner_send.at[0], pt_recv.at[slot % 2], partner
            ).start()

        for at, actions in after.items():

            @pl.when(t == at)
            def _():
                for a in actions:
                    a()

        return carry

    lax.fori_loop(0, STEPS, step, 0)

    for h in range(2):
        partner_term(6 + h).wait_recv()
    for h in range(2):
        far_term(h).wait_recv()
    for q in range(len(sums)):
        for h in range(2):
            add_rows(*sums[q], [acc.at[3 + h], partner_terms.at[6 + h], arrived.at[h]], terms.at[4 + h])
            sum_term(h, q).start()
    for h in range(2):
        plain_term(h).wait_recv()
        add_rows(0, half, [acc.at[1 + h], partner_terms.at[h], arrived.at[2 + h]], acc.at[1 + h])
    pltpu.make_async_copy(x_all, x_all, partner_send.at[0]).wait()
    for p in range(len(sums)):
        for h in range(2):
            sum_term(h, p).wait_recv()
            add_rows(*sums[p], [acc.at[1 + h], arrived.at[4 + h]], y_ref.at[pl.ds(h * half, half)])
    sent = x_all.at[pl.ds(0, 12)]
    pltpu.make_async_copy(sent, sent, ring_send.at[0]).wait()


def solution(mesh):
    n = mesh.shape["tp"]

    def step(x, w_gate, w_up, w_down):
        rows, depth = x.shape
        width = w_gate.shape[1]
        half = rows // 2
        dma = pltpu.SemaphoreType.DMA
        bf16 = jnp.bfloat16
        return pl.pallas_call(
            functools.partial(kernel, n),
            out_shape=pltpu.VMEM((rows, depth), bf16),
            in_specs=[pl.BlockSpec(memory_space=pl.ANY)] * 4,
            out_specs=pl.BlockSpec(memory_space=pltpu.VMEM),
            scratch_shapes=[
                pltpu.VMEM((STEPS, half, depth), bf16),
                pltpu.VMEM((depth, width), bf16),
                pltpu.VMEM((depth, width), bf16),
                pltpu.VMEM((width, depth), bf16),
                pltpu.VMEM((half, width), bf16),
                pltpu.VMEM((5, half, depth), F32),
                pltpu.VMEM((6, half, depth), bf16),
                pltpu.VMEM((SLOTS, half, depth), bf16),
                pltpu.VMEM((6, half, depth), bf16),
                dma((2, 2)),
                dma((1,)),
                dma((1,)),
                dma((1,)),
                dma((2, PIECES)),
                dma((2,)),
                dma((2,)),
                dma((2,)),
            ],
            compiler_params=pltpu.CompilerParams(
                collective_id=0, has_side_effects=True, vmem_limit_bytes=61 * 2**20
            ),
        )(x, w_gate, w_up, w_down)

    return jax.shard_map(
        step,
        mesh=mesh,
        in_specs=(P(("dp", "tp"), None), P(None, "tp"), P(None, "tp"), P("tp", None)),
        out_specs=P(("dp", "tp"), None),
        check_vma=False,
    )
```

```python
import functools

import jax
import jax.numpy as jnp
from jax import lax
from jax.experimental import pallas as pl
from jax.experimental.pallas import tpu as pltpu
from jax.sharding import PartitionSpec as P

F32 = jnp.float32
CORES = 2
PIECES = 2
FIRST = 64
LAST = 32
TILE = 256

SLOTS = 8
STEPS = 2 * SLOTS


def kernel(
    n, x_hbm, wg_hbm, wu_hbm, wd_hbm, y_ref,
    x_all, wg, wu, wd, hidden, acc, terms, partner_terms, arrived,
    hello, own_sem, weight_sem, ring_send, partner_send, near_recv, half_recv, relay_recv, pt_recv,
):
    half, depth = x_all.shape[1:]
    me = lax.axis_index("tp")
    right = {"tp": lax.rem(me + CORES, n)}
    left = {"tp": lax.rem(me + n - CORES, n)}
    partner = {"tp": me + 1 - 2 * lax.rem(me, CORES)}
    part = half // PIECES
    pieces = [pl.ds(p * part, part) for p in range(PIECES)]
    near = [(0, FIRST), (FIRST, half - FIRST)]
    whole = pl.ds(0, half)
    sums = [(0, half - LAST), (half - LAST, LAST)]

    def remote(src, dst, send, recv, device):
        return pltpu.make_async_remote_copy(
            src_ref=src, dst_ref=dst, send_sem=send, recv_sem=recv,
            device_id=device, device_id_type=pl.DeviceIdType.MESH,
        )

    def mine(slot):
        return 2 * slot + 1

    moves = [(0, right), (1, left), (2, right), (3, left), (0, left), (1, right)]

    def gather(slot, p=None, start=None):
        src, device = moves[slot - 2]
        rows = whole if p is None else pl.ds(*near[p])
        recv = near_recv.at[slot - 2, p] if slot < 4 else half_recv.at[slot - 4] if slot < 6 else own_sem.at[slot - 6, 0]
        origin = x_all.at[mine(src), rows] if start is None else start
        return remote(origin, x_all.at[mine(slot), rows], ring_send.at[0], recv, device)

    def relay(slot, rows=whole):
        return remote(
            x_all.at[mine(slot), rows], x_all.at[2 * slot, rows],
            partner_send.at[0], relay_recv.at[slot % 2], partner,
        )

    def partner_term(slot):
        return remote(
            x_all.at[2 * slot], partner_terms.at[slot], partner_send.at[0], pt_recv.at[slot % 2], partner
        )

    def far_term(h, rows=whole):
        return remote(
            terms.at[2 + h, rows], arrived.at[h, rows], ring_send.at[0], near_recv.at[1 - h, 0], (right, left)[h]
        )

    def plain_term(h):
        return remote(
            terms.at[h], arrived.at[2 + h], ring_send.at[0], near_recv.at[h, 1], (left, right)[h]
        )

    def sum_term(h, p):
        rows = pl.ds(*sums[p])
        recv = half_recv.at[h] if p == 0 else own_sem.at[h, 1]
        return remote(
            terms.at[4 + h, rows], arrived.at[4 + h, rows], ring_send.at[0], recv, (right, left)[h]
        )

    own = [
        pltpu.make_async_copy(
            x_hbm.at[pl.ds(h * half + start, size)], x_all.at[mine(h), pl.ds(start, size)], own_sem.at[h, p]
        )
        for p, (start, size) in enumerate(near)
        for h in range(2)
    ]
    weights = [
        pltpu.make_async_copy(src, dst, weight_sem.at[0])
        for src, dst in ((wg_hbm, wg), (wu_hbm, wu), (wd_hbm, wd))
    ]
    barrier = pltpu.get_barrier_semaphore()

    def greet(device):
        pl.semaphore_signal(barrier, inc=1, device_id=device, device_id_type=pl.DeviceIdType.MESH)

    core = lax.rem(me, CORES)
    greet(left)
    for c in own + weights:
        c.start()
    pl.semaphore_wait(barrier, 2 - core)
    pl.semaphore_signal(hello, inc=1, device_id=right, device_id_type=pl.DeviceIdType.MESH)
    for h in range(2):
        if h == 1:
            pl.semaphore_wait(hello, 1)
        gather(2 + h, 0, x_hbm.at[pl.ds(h * half, FIRST)]).start()
        if h == 0:
            greet(partner)
    for h in range(2):
        own[h].wait()
    for h in range(2):
        own[2 + h].wait()
        gather(2 + h, 1).start()

    @pl.when(core == 1)
    def _():
        pl.semaphore_wait(barrier, 1)

    for h in range(2):
        relay(h).start()
    def arrive_near(p):
        for slot in (2, 3):
            gather(slot, p).wait_recv()
            gather(slot + 2, p).start()
            relay(slot, pl.ds(*near[p])).start()

    def arrive_half(slots):
        for slot in slots:
            gather(slot).wait_recv()
            relay(slot).start()

    blocks = 3 * wg.shape[1] // half
    assert wd.shape == wg.shape[::-1] and blocks <= STEPS
    loaded = x_all.at[pl.ds(0, blocks)]

    def have_weights():
        pltpu.make_async_copy(loaded, loaded, weight_sem.at[0]).wait()

    def relayed(slot):
        relay(slot).wait_recv()

    def start_near2():
        for slot in (6, 7):
            gather(slot).start()

    def own_terms():
        for h in range(2):
            partner_term(h).wait_recv()

    before = {
        0: [lambda: relayed(0), have_weights],
        2: [lambda: relayed(1)],
        4: [own_terms, lambda: arrive_near(0), lambda: arrive_near(1), start_near2, lambda: relayed(2)],
        6: [lambda: relayed(3)],
        8: [lambda: arrive_half((4, 5)), lambda: relayed(4)],
        10: [lambda: relayed(5)],
        12: [lambda: arrive_half((6, 7)), lambda: relayed(6)],
        14: [lambda: relayed(7)],
    }

    def add_rows(start, size, srcs, dst):
        chunk = 32

        @pl.loop(0, size // chunk)
        def _(i):
            r = pl.ds(pl.multiple_of(start + i * chunk, chunk), chunk)
            total = srcs[0][r, :].astype(F32)
            for s in srcs[1:]:
                total += s[r, :].astype(F32)
            dst[r, :] = total.astype(dst.dtype)

    def finish_far(h):
        partner_term(4 + h).wait_recv()
        for p in range(PIECES):
            add_rows(p * part, part, [acc.at[0], partner_terms.at[4 + h]], terms.at[2 + h])
            far_term(h, pieces[p]).start()

    def finish_plain(h):
        partner_term(2 + h).wait_recv()
        add_rows(0, half, [acc.at[0], partner_terms.at[2 + h]], terms.at[h])

    def start_plain():
        for h in range(2):
            plain_term(h).start()

    after = {
        5: [lambda: finish_plain(0)],
        7: [lambda: finish_plain(1)],
        9: [lambda: finish_far(0)],
        11: [lambda: finish_far(1), start_plain],
    }

    def step(t, carry):
        for at, actions in before.items():

            @pl.when(t == at)
            def _():
                for a in actions:
                    a()

        rows_in = x_all.at[t]
        for c in range(0, hidden.shape[1], TILE):
            cols = pl.ds(c, TILE)
            gate = jnp.dot(rows_in[...], wg[:, cols], preferred_element_type=F32)
            up = jnp.dot(rows_in[...], wu[:, cols], preferred_element_type=F32)
            hidden[:, cols] = (jax.nn.silu(gate) * up).astype(hidden.dtype)
        slot = t // 2
        to = (t % 2) * (jnp.where(slot < 2, slot + 1, 0) + jnp.where(slot > 5, slot - 3, 0))
        for c in range(0, depth, TILE):
            cols = pl.ds(c, TILE)
            acc[to, :, cols] = jnp.dot(hidden[...], wd[:, cols], preferred_element_type=F32)

        @pl.when(t % 2 == 0)
        def _():
            add_rows(0, half, [acc.at[0]], x_all.at[t])
            remote(
                x_all.at[t], partner_terms.at[slot], partner_send.at[0], pt_recv.at[slot % 2], partner
            ).start()

        for at, actions in after.items():

            @pl.when(t == at)
            def _():
                for a in actions:
                    a()

        return carry

    lax.fori_loop(0, STEPS, step, 0)

    for h in range(2):
        partner_term(6 + h).wait_recv()
    for h in range(2):
        far_term(h).wait_recv()
    for q in range(len(sums)):
        for h in range(2):
            add_rows(*sums[q], [acc.at[3 + h], partner_terms.at[6 + h], arrived.at[h]], terms.at[4 + h])
            sum_term(h, q).start()
    for h in range(2):
        plain_term(h).wait_recv()
        add_rows(0, half, [acc.at[1 + h], partner_terms.at[h], arrived.at[2 + h]], acc.at[1 + h])
    pltpu.make_async_copy(x_all, x_all, partner_send.at[0]).wait()
    for p in range(len(sums)):
        for h in range(2):
            sum_term(h, p).wait_recv()
            add_rows(*sums[p], [acc.at[1 + h], arrived.at[4 + h]], y_ref.at[pl.ds(h * half, half)])
    sent = x_all.at[pl.ds(0, 12)]
    pltpu.make_async_copy(sent, sent, ring_send.at[0]).wait()


def solution(mesh):
    n = mesh.shape["tp"]

    def step(x, w_gate, w_up, w_down):
        rows, depth = x.shape
        width = w_gate.shape[1]
        half = rows // 2
        dma = pltpu.SemaphoreType.DMA
        bf16 = jnp.bfloat16
        return pl.pallas_call(
            functools.partial(kernel, n),
            out_shape=pltpu.VMEM((rows, depth), bf16),
            in_specs=[pl.BlockSpec(memory_space=pl.ANY)] * 4,
            out_specs=pl.BlockSpec(memory_space=pltpu.VMEM),
            scratch_shapes=[
                pltpu.VMEM((STEPS, half, depth), bf16),
                pltpu.VMEM((depth, width), bf16),
                pltpu.VMEM((depth, width), bf16),
                pltpu.VMEM((width, depth), bf16),
                pltpu.VMEM((half, width), bf16),
                pltpu.VMEM((5, half, depth), F32),
                pltpu.VMEM((6, half, depth), bf16),
                pltpu.VMEM((SLOTS, half, depth), bf16),
                pltpu.VMEM((6, half, depth), bf16),
                pltpu.SemaphoreType.REGULAR,
                dma((2, 2)),
                dma((1,)),
                dma((1,)),
                dma((1,)),
                dma((2, PIECES)),
                dma((2,)),
                dma((2,)),
                dma((2,)),
            ],
            compiler_params=pltpu.CompilerParams(
                collective_id=0, has_side_effects=True, vmem_limit_bytes=61 * 2**20
            ),
        )(x, w_gate, w_up, w_down)

    return jax.shard_map(
        step,
        mesh=mesh,
        in_specs=(P(("dp", "tp"), None), P(None, "tp"), P(None, "tp"), P("tp", None)),
        out_specs=P(("dp", "tp"), None),
        check_vma=False,
    )
```

```python
import functools

import jax
import jax.numpy as jnp
from jax import lax
from jax.experimental import pallas as pl
from jax.experimental.pallas import tpu as pltpu
from jax.sharding import PartitionSpec as P

F32 = jnp.float32
CORES = 2
PIECES = 2
FIRST = 64
LAST = 32
TILE = 256

SLOTS = 8
STEPS = 2 * SLOTS


def kernel(
    n, x_hbm, wg_hbm, wu_hbm, wd_hbm, y_ref,
    x_all, wg, wu, wd, hidden, acc, terms, partner_terms, arrived,
    hello, own_sem, weight_sem, ring_send, partner_send, near_recv, half_recv, relay_recv, pt_recv,
):
    half, depth = x_all.shape[1:]
    me = lax.axis_index("tp")
    right = {"tp": lax.rem(me + CORES, n)}
    left = {"tp": lax.rem(me + n - CORES, n)}
    partner = {"tp": me + 1 - 2 * lax.rem(me, CORES)}
    part = half // PIECES
    pieces = [pl.ds(p * part, part) for p in range(PIECES)]
    near = [(0, FIRST), (FIRST, half - FIRST)]
    whole = pl.ds(0, half)
    sums = [(0, half - LAST), (half - LAST, LAST)]

    def remote(src, dst, send, recv, device):
        return pltpu.make_async_remote_copy(
            src_ref=src, dst_ref=dst, send_sem=send, recv_sem=recv,
            device_id=device, device_id_type=pl.DeviceIdType.MESH,
        )

    def mine(slot):
        return 2 * slot + 1

    moves = [(0, right), (1, left), (2, right), (3, left), (0, left), (1, right)]

    def gather(slot, p=None, start=None):
        src, device = moves[slot - 2]
        rows = whole if p is None else pl.ds(*near[p])
        recv = near_recv.at[slot - 2, p] if slot < 4 else half_recv.at[slot - 4] if slot < 6 else own_sem.at[slot - 6, 0]
        origin = x_all.at[mine(src), rows] if start is None else start
        return remote(origin, x_all.at[mine(slot), rows], ring_send.at[0], recv, device)

    def relay(slot, rows=whole):
        return remote(
            x_all.at[mine(slot), rows], x_all.at[2 * slot, rows],
            partner_send.at[0], relay_recv.at[slot % 2], partner,
        )

    def partner_term(slot):
        return remote(
            x_all.at[2 * slot], partner_terms.at[slot], partner_send.at[0], pt_recv.at[slot % 2], partner
        )

    def far_term(h, rows=whole):
        return remote(
            terms.at[2 + h, rows], arrived.at[h, rows], ring_send.at[0], near_recv.at[1 - h, 0], (right, left)[h]
        )

    def plain_term(h):
        return remote(
            terms.at[h], arrived.at[2 + h], ring_send.at[0], near_recv.at[h, 1], (left, right)[h]
        )

    def sum_term(h, p):
        rows = pl.ds(*sums[p])
        recv = half_recv.at[h] if p == 0 else own_sem.at[h, 1]
        return remote(
            terms.at[4 + h, rows], arrived.at[4 + h, rows], ring_send.at[0], recv, (right, left)[h]
        )

    own = [
        pltpu.make_async_copy(
            x_hbm.at[pl.ds(h * half + start, size)], x_all.at[mine(h), pl.ds(start, size)], own_sem.at[h, p]
        )
        for p, (start, size) in enumerate(near)
        for h in range(2)
    ]
    weights = [
        pltpu.make_async_copy(src, dst, weight_sem.at[0])
        for src, dst in ((wg_hbm, wg), (wu_hbm, wu), (wd_hbm, wd))
    ]
    barrier = pltpu.get_barrier_semaphore()

    def greet(device):
        pl.semaphore_signal(barrier, inc=1, device_id=device, device_id_type=pl.DeviceIdType.MESH)

    core = lax.rem(me, CORES)
    greet(left)
    pl.semaphore_wait(barrier, 2 - core)
    gather(2, 0, x_hbm.at[pl.ds(0, FIRST)]).start()
    pl.semaphore_signal(hello, inc=1, device_id=right, device_id_type=pl.DeviceIdType.MESH)
    greet(partner)
    for c in own + weights:
        c.start()
    pl.semaphore_wait(hello, 1)
    gather(3, 0, x_hbm.at[pl.ds(half, FIRST)]).start()
    for h in range(2):
        own[h].wait()
    for h in range(2):
        own[2 + h].wait()
        gather(2 + h, 1).start()

    @pl.when(core == 1)
    def _():
        pl.semaphore_wait(barrier, 1)

    for h in range(2):
        relay(h).start()
    def arrive_near(p):
        for slot in (2, 3):
            gather(slot, p).wait_recv()
            gather(slot + 2, p).start()
            relay(slot, pl.ds(*near[p])).start()

    def arrive_half(slots):
        for slot in slots:
            gather(slot).wait_recv()
            relay(slot).start()

    blocks = 3 * wg.shape[1] // half
    assert wd.shape == wg.shape[::-1] and blocks <= STEPS
    loaded = x_all.at[pl.ds(0, blocks)]

    def have_weights():
        pltpu.make_async_copy(loaded, loaded, weight_sem.at[0]).wait()

    def relayed(slot):
        relay(slot).wait_recv()

    def start_near2():
        for slot in (6, 7):
            gather(slot).start()

    def own_terms():
        for h in range(2):
            partner_term(h).wait_recv()

    before = {
        0: [lambda: relayed(0), have_weights],
        2: [lambda: relayed(1)],
        4: [own_terms, lambda: arrive_near(0), lambda: arrive_near(1), start_near2, lambda: relayed(2)],
        6: [lambda: relayed(3)],
        8: [lambda: arrive_half((4, 5)), lambda: relayed(4)],
        10: [lambda: relayed(5)],
        12: [lambda: arrive_half((6, 7)), lambda: relayed(6)],
        14: [lambda: relayed(7)],
    }

    def add_rows(start, size, srcs, dst):
        chunk = 32

        @pl.loop(0, size // chunk)
        def _(i):
            r = pl.ds(pl.multiple_of(start + i * chunk, chunk), chunk)
            total = srcs[0][r, :].astype(F32)
            for s in srcs[1:]:
                total += s[r, :].astype(F32)
            dst[r, :] = total.astype(dst.dtype)

    def finish_far(h):
        partner_term(4 + h).wait_recv()
        for p in range(PIECES):
            add_rows(p * part, part, [acc.at[0], partner_terms.at[4 + h]], terms.at[2 + h])
            far_term(h, pieces[p]).start()

    def finish_plain(h):
        partner_term(2 + h).wait_recv()
        add_rows(0, half, [acc.at[0], partner_terms.at[2 + h]], terms.at[h])

    def start_plain():
        for h in range(2):
            plain_term(h).start()

    after = {
        5: [lambda: finish_plain(0)],
        7: [lambda: finish_plain(1)],
        9: [lambda: finish_far(0)],
        11: [lambda: finish_far(1), start_plain],
    }

    def step(t, carry):
        for at, actions in before.items():

            @pl.when(t == at)
            def _():
                for a in actions:
                    a()

        rows_in = x_all.at[t]
        for c in range(0, hidden.shape[1], TILE):
            cols = pl.ds(c, TILE)
            gate = jnp.dot(rows_in[...], wg[:, cols], preferred_element_type=F32)
            up = jnp.dot(rows_in[...], wu[:, cols], preferred_element_type=F32)
            hidden[:, cols] = (jax.nn.silu(gate) * up).astype(hidden.dtype)
        slot = t // 2
        to = (t % 2) * (jnp.where(slot < 2, slot + 1, 0) + jnp.where(slot > 5, slot - 3, 0))
        for c in range(0, depth, TILE):
            cols = pl.ds(c, TILE)
            acc[to, :, cols] = jnp.dot(hidden[...], wd[:, cols], preferred_element_type=F32)

        @pl.when(t % 2 == 0)
        def _():
            add_rows(0, half, [acc.at[0]], x_all.at[t])
            remote(
                x_all.at[t], partner_terms.at[slot], partner_send.at[0], pt_recv.at[slot % 2], partner
            ).start()

        for at, actions in after.items():

            @pl.when(t == at)
            def _():
                for a in actions:
                    a()

        return carry

    lax.fori_loop(0, STEPS, step, 0)

    for h in range(2):
        partner_term(6 + h).wait_recv()
    for h in range(2):
        far_term(h).wait_recv()
    for q in range(len(sums)):
        for h in range(2):
            add_rows(*sums[q], [acc.at[3 + h], partner_terms.at[6 + h], arrived.at[h]], terms.at[4 + h])
            sum_term(h, q).start()
    for h in range(2):
        plain_term(h).wait_recv()
        add_rows(0, half, [acc.at[1 + h], partner_terms.at[h], arrived.at[2 + h]], acc.at[1 + h])
    pltpu.make_async_copy(x_all, x_all, partner_send.at[0]).wait()
    for p in range(len(sums)):
        for h in range(2):
            sum_term(h, p).wait_recv()
            add_rows(*sums[p], [acc.at[1 + h], arrived.at[4 + h]], y_ref.at[pl.ds(h * half, half)])
    sent = x_all.at[pl.ds(0, 12)]
    pltpu.make_async_copy(sent, sent, ring_send.at[0]).wait()


def solution(mesh):
    n = mesh.shape["tp"]

    def step(x, w_gate, w_up, w_down):
        rows, depth = x.shape
        width = w_gate.shape[1]
        half = rows // 2
        dma = pltpu.SemaphoreType.DMA
        bf16 = jnp.bfloat16
        return pl.pallas_call(
            functools.partial(kernel, n),
            out_shape=pltpu.VMEM((rows, depth), bf16),
            in_specs=[pl.BlockSpec(memory_space=pl.ANY)] * 4,
            out_specs=pl.BlockSpec(memory_space=pltpu.VMEM),
            scratch_shapes=[
                pltpu.VMEM((STEPS, half, depth), bf16),
                pltpu.VMEM((depth, width), bf16),
                pltpu.VMEM((depth, width), bf16),
                pltpu.VMEM((width, depth), bf16),
                pltpu.VMEM((half, width), bf16),
                pltpu.VMEM((5, half, depth), F32),
                pltpu.VMEM((6, half, depth), bf16),
                pltpu.VMEM((SLOTS, half, depth), bf16),
                pltpu.VMEM((6, half, depth), bf16),
                pltpu.SemaphoreType.REGULAR,
                dma((2, 2)),
                dma((1,)),
                dma((1,)),
                dma((1,)),
                dma((2, PIECES)),
                dma((2,)),
                dma((2,)),
                dma((2,)),
            ],
            compiler_params=pltpu.CompilerParams(
                collective_id=0, has_side_effects=True, vmem_limit_bytes=61 * 2**20
            ),
        )(x, w_gate, w_up, w_down)

    return jax.shard_map(
        step,
        mesh=mesh,
        in_specs=(P(("dp", "tp"), None), P(None, "tp"), P(None, "tp"), P("tp", None)),
        out_specs=P(("dp", "tp"), None),
        check_vma=False,
    )
```
